256 devices in a mesh: row: 32 (over y, z), col: 8 (over x, core).
Axes of the slice: x: 4, y: 4, z: 8, core: 2. Of those that a mesh axis runs over, the one named last changes fastest.
Arguments:
- grams: bfloat16 [4, 3584, 3584], P(None, 'row', 'col'), as said below
- weights: bfloat16 [4, 3584, 7168], P(None, 'row', 'col'), may hold values from -6 to 6
Outputs:
- merged: float32 [3584, 7168], P('row', 'col')
- residual: float32 [3584, 7168], P('row', 'col')
The draws below stay inside these ranges and needn't reach their ends.
Inputs may be any that keep to these rules, and one draw needn't show every extreme that they name: `grams`: each of the 4 matrices is symmetric and positive definite.
All inputs are finite; a program needn't handle non-finite values.
Results may differ from the reference program's by a relative error of at most 0.012.
The reference program's roundings to bfloat16 on the way (of `rounded`) count: a program that leaves them out, or rounds other values in their place, can miss the bound.
Values may be sent and summed in bfloat16 or wider, within the bound.
A program may use at most 256 MiB of HBM per device.

```python
import math
import jax
import jax.numpy as jnp
from jax import lax

D = 3584
FF_COLS = 7168
MODELS = 4
ITERS = 2


def draw_grams(key, part):

    def one_model(model_key):
        scale_key, noise_key = jax.random.split(model_key)
        lowest, highest, spread = (0.5, 5.0, 0.3)
        scales = jnp.exp(jax.random.uniform(scale_key, (D,), jnp.float32, math.log(lowest), math.log(highest)))
        roots = jnp.sqrt(scales)
        noise = jax.random.normal(noise_key, (D, D), jnp.float32) * (spread / math.sqrt(D))
        core = jnp.eye(D, dtype=jnp.float32) + (noise + noise.T) * 0.5
        return (core * (roots[:, None] * roots[None, :])).astype(jnp.bfloat16)
    model_keys = jax.random.split(jax.random.fold_in(key, 17), MODELS)
    return jax.vmap(one_model)(model_keys)


def shard_levels(stream_key, shape, cuts, smallest, high):
    def one(position, parts):
        draws = jax.random.uniform(jax.random.fold_in(jax.random.fold_in(stream_key, 6), position), (parts,), jnp.float32, smallest / len(cuts), high / len(cuts))
        return jnp.repeat(jnp.exp(draws), shape[position] // parts).reshape((-1,) + (1,) * (len(shape) - position - 1))

    factor_of = one(*cuts[0])
    for cut in cuts[1:]:
        factor_of = factor_of * one(*cut)
    return factor_of


def bell_draw(rng, shape, width, limit, pieces=(), kind=jnp.bfloat16):
    factor_of = shard_levels(rng, shape, pieces, -0.22, 0.18) if pieces else 1.0
    values = jax.random.normal(rng, shape, jnp.float32) * width * factor_of
    return jnp.minimum(jnp.maximum(values, -limit), limit).astype(kind)


def setup_inputs(seed: int = 0) -> dict:
    streams_of = jax.random.split(jax.random.key(seed), 3)
    return {
        "grams": draw_grams(jax.random.fold_in(streams_of[2], 71), 0),
        "weights": bell_draw(streams_of[1], (MODELS, D, FF_COLS), 1.0, 6.0, ((1, 32), (2, 8))),
    }


def reference(grams, weights):
    high = lax.Precision.HIGHEST
    total = jnp.zeros((D, D), jnp.float32)
    right_side = jnp.zeros((D, FF_COLS), jnp.float32)
    for model_index in range(MODELS):
        gram_full = grams[model_index].astype(jnp.float32)
        weight = weights[model_index].astype(jnp.float32)
        gram_diag = jnp.diagonal(gram_full)
        right_side = right_side + 0.9 * jnp.dot(gram_full, weight, precision=high) + 0.1 * gram_diag[:, None] * weight
        total = total + gram_full
    total_diag = jnp.diagonal(total)
    merged = jnp.zeros((D, FF_COLS), jnp.float32)
    residual = right_side
    direction = right_side
    norm_now = jnp.sum(residual * residual, axis=0)
    for iteration in range(ITERS):
        rounded = lax.optimization_barrier(direction.astype(jnp.bfloat16)).astype(jnp.float32)
        mapped = 0.9 * jnp.dot(total, rounded, precision=high) + 0.1 * total_diag[:, None] * rounded
        curvature = jnp.sum(direction * mapped, axis=0)
        step_length = norm_now / curvature
        merged = merged + step_length * direction
        residual = residual - step_length * mapped
        if iteration + 1 < ITERS:
            norm_next = jnp.sum(residual * residual, axis=0)
            direction = residual + (norm_next / norm_now) * direction
            norm_now = norm_next
    return merged, residual
```

```python
import functools

import jax
import jax.numpy as jnp
from jax import lax
from jax.experimental import pallas as pl
from jax.experimental.pallas import tpu as pltpu
from jax.sharding import Mesh
from jax.sharding import PartitionSpec as P

MESH = pl.DeviceIdType.MESH
F32 = jnp.float32
BF16 = jnp.bfloat16

NX, NY, NZ = 4, 4, 8
M = 4
R = 112
LANES = 128
HALF = 4 * R
CHUNKS = 7
F_LO, F_HI = pl.ds(0, 56), pl.ds(56, 56)
B_LO, B_HI = pl.ds(0, 64), pl.ds(64, 48)

RSZ = 0
AGZ = 8
RSY = 24
STY = 32
STZ = 38
KINDS = 52


def kernel(
    g_ref,
    w_ref,
    merged_ref,
    resid_ref,
    gt,
    t_hi,
    t_lo,
    diag,
    wb,
    cb,
    rz,
    d1,
    d2,
    pb,
    ry,
    res,
    dirn,
    mapped,
    merged,
    sty,
    stz,
    q_send,
    q_recv,
    e_send,
    e_recv,
    w_send,
    w_recv,
    s_send,
    s_recv,
):
    x, y, z, c = (lax.axis_index(a) for a in ("x", "y", "z", "c"))
    other = 1 - c
    z_half, z_quarter = lax.div(z, 4), lax.rem(z, 4)
    home = z_half == c

    def at(axis, index, step, size):
        return {axis: lax.rem(index + (step + size), size)}

    xp, xm = at("x", x, 1, NX), at("x", x, -1, NX)
    yp, ym = at("y", y, 1, NY), at("y", y, -1, NY)
    zp, zm = at("z", z, 1, NZ), at("z", z, -1, NZ)

    def zi(step):
        return lax.rem(z + (step + NZ), NZ)

    def yi(step):
        return lax.rem(y + (step + NY), NY)

    def xi(step):
        return lax.rem(x + (step + NX), NX)

    def copy(src, dst, send, recv, device):
        return pltpu.make_async_remote_copy(
            src_ref=src, dst_ref=dst, send_sem=send, recv_sem=recv, device_id=device, device_id_type=MESH
        )

    barrier = pltpu.get_barrier_semaphore()
    for dz in range(NZ):
        for dc in range(2):
            if dz or dc:
                pl.semaphore_signal(
                    barrier, inc=1, device_id={"z": zi(dz), "c": lax.rem(c + dc, 2)}, device_id_type=MESH
                )
    for d in (1, 2, 3):
        pl.semaphore_signal(barrier, inc=1, device_id=at("y", y, d, NY), device_id_type=MESH)
    for device in (xp, xm):
        pl.semaphore_signal(barrier, inc=1, device_id=device, device_id_type=MESH)
    pl.semaphore_wait(barrier, 2 * NZ - 1 + 3 + 2)

    def w_copy(j, way):
        lanes = pl.ds(j * LANES, LANES)
        return copy(
            w_ref.at[:, :, lanes], wb.at[j, y, :, pl.ds(0, R), :], w_send.at[way, j], w_recv.at[way, j], (yp, ym)[way]
        )

    def w_arrival(j, way):
        dst = wb.at[j, yi(-1 if way == 0 else 1), :, pl.ds(0, R), :]
        return copy(dst, dst, w_send.at[way, j], w_recv.at[way, j], (yp, ym)[way])

    def w_forward(j, way):
        models = pl.ds(0, 2) if way == 0 else pl.ds(2, 2)
        dst = wb.at[j, yi(-1 if way == 0 else 1), models, pl.ds(0, R), :]
        return copy(dst, dst, w_send.at[2 + way, j], w_recv.at[2 + way, j], (yp, ym)[way])

    def w_far(j, way):
        models = pl.ds(0, 2) if way == 0 else pl.ds(2, 2)
        dst = wb.at[j, yi(2), models, pl.ds(0, R), :]
        return copy(dst, dst, w_send.at[2 + way, j], w_recv.at[2 + way, j], (yp, ym)[way])

    def q_copy(m, quarter):
        return copy(
            g_ref.at[quarter, m],
            gt.at[z_half, x, m, pl.ds(pl.multiple_of(z_quarter * R, 16), R), :],
            q_send.at[m, quarter],
            q_recv.at[m, z_quarter],
            {"z": 4 * c + quarter, "c": z_half},
        )

    def q_arrival(m, quarter):
        dst = gt.at[c, x, m, pl.ds(quarter * R, R), :]
        return copy(dst, dst, q_send.at[m, quarter], q_recv.at[m, quarter], {"z": 4 * c + quarter, "c": z_half})

    def away(quarter):
        return jnp.logical_not(jnp.logical_and(home, z_quarter == quarter))

    for m in range(M):
        for quarter in range(4):

            @pl.when(away(quarter))
            def _():
                q_copy(m, quarter).start()

    for j in range(CHUNKS):
        for way in range(2):
            w_copy(j, way).start()

    @pl.when(home)
    def _():
        rows = pl.ds(pl.multiple_of(z_quarter * R, 16), R)
        for m in range(M):
            gt[z_half, x, m, rows, :] = g_ref[z_quarter, m]

    for j in range(CHUNKS):
        for m in range(M):
            wb[j, y, m, pl.ds(0, R), :] = w_ref[m, :, j * LANES : (j + 1) * LANES]
            for k in range(NY):
                wb[j, k, m, pl.ds(R, LANES - R), :] = jnp.zeros((LANES - R, LANES), BF16)

    def e_copy(m, offset, kind, device):
        ref = gt.at[c, xi(offset), m]
        return copy(ref, ref, e_send.at[kind, m], e_recv.at[kind, m], device)

    def e_from_core(m, k):
        ref = gt.at[other, xi(k), m]
        return copy(ref, ref, e_send.at[3 + k, m], e_recv.at[3 + k, m], {"c": other})

    def to_core(m, k):
        return e_copy(m, k, 3 + k, {"c": other})

    for m in range(M):
        for quarter in range(4):

            @pl.when(away(quarter))
            def _():
                q_arrival(m, quarter).wait_recv()

        e_copy(m, 0, 0, xp).start()
        e_copy(m, 0, 1, xm).start()
        to_core(m, 0).start()
    for j in range(2):
        for way in range(2):
            w_arrival(j, way).wait_recv()
            w_forward(j, way).start()
    for m in (0, 2, 1, 3):
        e_copy(m, -1, 0, xp).wait_recv()
        if m < 2:
            e_copy(m, -1, 2, xp).start()
        to_core(m, 3).start()
        e_copy(m, 1, 1, xm).wait_recv()
        if m >= 2:
            e_copy(m, 1, 2, xm).start()
        to_core(m, 1).start()
    for j in range(2, CHUNKS):
        for way in range(2):
            w_arrival(j, way).wait_recv()
            w_forward(j, way).start()
    for m in (0, 2, 1, 3):
        e_copy(m, 2, 2, xp).wait_recv()
        to_core(m, 2).start()
    for m in range(M):
        for k in range(NX):
            e_from_core(m, k).wait_recv()

    for k in range(NX):
        total = jnp.concatenate(
            [
                gt[h, k, 0].astype(F32) + gt[h, k, 1].astype(F32) + gt[h, k, 2].astype(F32) + gt[h, k, 3].astype(F32)
                for h in range(2)
            ],
            axis=0,
        )
        total = jnp.transpose(total)[:R]
        high = total.astype(BF16)
        t_hi[k * R : (k + 1) * R, :] = high
        t_lo[k * R : (k + 1) * R, :] = (total - high.astype(F32)).astype(BF16)
    on_diag = lax.broadcasted_iota(jnp.int32, (R, LANES), 0) == lax.broadcasted_iota(jnp.int32, (R, LANES), 1)
    diag_total = jnp.zeros((R, LANES), F32)
    for m in range(M):
        block = gt[z_half, y, m, pl.ds(pl.multiple_of(z_quarter * R, 16), R), :].astype(F32)
        values = jnp.sum(jnp.where(on_diag, block, 0.0), axis=1, keepdims=True)
        values = jnp.broadcast_to(values, (R, LANES))
        diag[m] = values
        diag_total = diag_total + values
    diag[M] = diag_total

    def message(kind, j, src, dst, device):
        return copy(src, dst, s_send.at[kind], s_recv.at[kind, j], device)

    def arrived(kind, j, dst, device):
        copy(dst, dst, s_send.at[kind], s_recv.at[kind, j], device).wait_recv()

    def sent(kind, j, src, device):
        copy(src, src, s_send.at[kind], s_recv.at[kind, j], device).wait_send()

    def rsz(j, step, way):
        sign = 1 if way == 0 else -1
        t = zi(sign * (5 - step))
        rows = pl.ds(0, R) if step > 1 else (F_LO, F_HI)[way]
        kind = RSZ + 2 * (step - 1) + way
        return kind, cb.at[j, t, rows, :], rz.at[way, j, step - 1, rows, :], (zp, zm)[way]

    def rsz_start(j, step):
        for way in range(2):
            kind, src, dst, device = rsz(j, step, way)
            message(kind, j, src, dst, device).start()

    def rsz_wait(j, step):
        for way in range(2):
            kind, src, dst, device = rsz(j, step, way)
            arrived(kind, j, dst, device)
            sent(kind, j, src, device)

    def right_partial(j):
        for way in range(2):
            w_far(j, way).wait_recv()
        for h in range(2):
            acc = jnp.zeros((HALF, LANES), F32)
            for k in range(NY):
                for m in (0, 2):
                    lhs = jnp.concatenate([gt[h, k, m], gt[h, k, m + 1]], axis=1)
                    rhs = jnp.concatenate([wb[j, k, m], wb[j, k, m + 1]], axis=0)
                    acc = acc + jnp.dot(lhs, rhs, preferred_element_type=F32)
            for q in range(4):
                cb[j, 4 * h + q] = acc[q * R : (q + 1) * R]
        rsz_start(j, 1)

    def right_step(step, j):
        rsz_wait(j, step - 1)
        plus, minus = zi(5 - step), zi(step - 5)
        if step == 2:
            cb[j, plus, F_LO, :] += rz[0, j, 0, F_LO, :]
            cb[j, minus, F_HI, :] += rz[1, j, 0, F_HI, :]
        else:
            cb[j, plus] += rz[0, j, step - 2]
            cb[j, minus] += rz[1, j, step - 2]
        rsz_start(j, step)

    def own_rows(index):
        return pl.multiple_of(index * R, 16)

    def agz(it, j, step, way, arriving):
        sign = -1 if way == 0 else 1
        origin = zi(sign * (step if arriving else step - 1))
        first, count = (0, R) if step < 4 else ((0, 64), (64, 48))[way]
        kind = AGZ + 8 * it + 2 * (step - 1) + way
        ref = (d1, d2)[it].at[j, pl.ds(pl.multiple_of(origin * R + first, 16), count), :]
        return kind, ref, (zp, zm)[way]

    def agz_start(it, j, step):
        for way in range(2):
            kind, ref, device = agz(it, j, step, way, False)
            message(kind, j, ref, ref, device).start()

    def agz_wait(it, j, step):
        for way in range(2):
            kind, ref, device = agz(it, j, step, way, True)
            arrived(kind, j, ref, device)
            kind, ref, device = agz(it, j, step, way, False)
            sent(kind, j, ref, device)

    def right_end(j):
        rsz_wait(j, 4)
        product = cb[j, z] + rz[0, j, 3] + rz[1, j, 3]
        on_diag_sum = jnp.zeros((R, LANES), F32)
        for m in range(M):
            on_diag_sum = on_diag_sum + diag[m] * wb[j, y, m, pl.ds(0, R), :].astype(F32)
        right = 0.9 * product + 0.1 * on_diag_sum
        res[j] = right
        dirn[j] = right
        d1[j, pl.ds(own_rows(z), R), :] = right.astype(BF16)
        agz_start(0, j, 1)

    def pass_on(it, step, j):
        agz_wait(it, j, step - 1)
        agz_start(it, j, step)

    def rsy(it, j, step, way):
        t = yi(2 if step == 1 else (1 if way == 0 else -1))
        rows = pl.ds(0, R) if step > 1 else (F_LO, F_HI)[way]
        kind = RSY + 4 * it + 2 * (step - 1) + way
        return kind, pb.at[it, j, t, rows, :], ry.at[it, way, j, step - 1, rows, :], (yp, ym)[way]

    def rsy_start(it, j, step):
        for way in range(2):
            kind, src, dst, device = rsy(it, j, step, way)
            message(kind, j, src, dst, device).start()

    def rsy_wait(it, j, step):
        for way in range(2):
            kind, src, dst, device = rsy(it, j, step, way)
            arrived(kind, j, dst, device)
            sent(kind, j, src, device)

    def map_partial(it, j):
        agz_wait(it, j, 4)
        d = (d1, d2)[it][j]
        out = jnp.dot(t_hi[...], d, preferred_element_type=F32) + jnp.dot(t_lo[...], d, preferred_element_type=F32)
        for q in range(NY):
            pb[it, j, q] = out[q * R : (q + 1) * R]
        rsy_start(it, j, 1)

    def map_step(it, j):
        rsy_wait(it, j, 1)
        pb[it, j, yi(1), F_LO, :] += ry[it, 0, j, 0, F_LO, :]
        pb[it, j, yi(-1), F_HI, :] += ry[it, 1, j, 0, F_HI, :]
        rsy_start(it, j, 2)

    def sty_message(it, j, d):
        return STY + 3 * it + d - 1, sty.at[it, j, y], at("y", y, d, NY)

    def stz_message(it, j, d):
        return STZ + 7 * it + d - 1, stz.at[it, j, z], at("z", z, d, NZ)

    def map_end(it, j):
        rsy_wait(it, j, 2)
        product = pb[it, j, y] + ry[it, 0, j, 1] + ry[it, 1, j, 1]
        rounded = (d1, d2)[it][j, pl.ds(own_rows(z), R), :].astype(F32)
        value = 0.9 * product + 0.1 * diag[M] * rounded
        mapped[j] = value
        r = res[j]
        norm = jnp.sum(r * r, axis=0, keepdims=True)
        curvature = jnp.sum(dirn[j] * value, axis=0, keepdims=True)
        square = jnp.sum(value * value, axis=0, keepdims=True)
        cross = jnp.sum(r * value, axis=0, keepdims=True)
        sty[it, j, y] = jnp.concatenate([norm, curvature, square, cross], axis=0)
        for d in (1, 2, 3):
            kind, ref, device = sty_message(it, j, d)
            message(kind, j, ref, ref, device).start()

    def sum_z(it, j):
        for d in (1, 2, 3):
            kind, ref, device = sty_message(it, j, d)
            arrived(kind, j, sty.at[it, j, yi(-d)], device)
            sent(kind, j, ref, device)
        stz[it, j, z] = (sty[it, j, 0] + sty[it, j, 1]) + (sty[it, j, 2] + sty[it, j, 3])
        for d in range(1, NZ):
            kind, ref, device = stz_message(it, j, d)
            message(kind, j, ref, ref, device).start()

    def update(it, j):
        for d in range(1, NZ):
            kind, ref, device = stz_message(it, j, d)
            arrived(kind, j, stz.at[it, j, zi(-d)], device)
            sent(kind, j, ref, device)
        sums = stz[it, j, 0]
        for k in range(1, NZ):
            sums = sums + stz[it, j, k]
        norm, curvature, square, cross = (sums[k : k + 1] for k in range(4))
        step = norm / curvature
        direction = dirn[j]
        residual = res[j] - step * mapped[j]
        if it == 0:
            norm_next = norm - 2.0 * step * cross + step * step * square
            merged[j] = step * direction
            direction = residual + norm_next / norm * direction
            res[j] = residual
            dirn[j] = direction
            d2[j, pl.ds(own_rows(z), R), :] = direction.astype(BF16)
            agz_start(1, j, 1)
        else:
            lanes = pl.ds(pl.multiple_of(j * LANES, LANES), LANES)
            merged_ref[:, lanes] = merged[j] + step * direction
            resid_ref[:, lanes] = residual

    stages = [right_partial]
    stages += [functools.partial(right_step, step) for step in (2, 3, 4)]
    stages += [right_end]
    for it in range(2):
        stages += [functools.partial(pass_on, it, step) for step in (2, 3, 4)]
        stages += [functools.partial(f, it) for f in (map_partial, map_step, map_end, sum_z, update)]

    def tick(t, carry):
        for s in reversed(range(len(stages))):
            j = t - s

            @pl.when(jnp.logical_and(j >= 0, j < CHUNKS))
            def _():
                stages[s](j)

        return carry

    lax.fori_loop(0, CHUNKS + len(stages) - 1, tick, 0)

    for m in range(M):
        for quarter in range(4):

            @pl.when(away(quarter))
            def _():
                q_copy(m, quarter).wait_send()

        e_copy(m, 0, 0, xp).wait_send()
        e_copy(m, 0, 1, xm).wait_send()
        if m < 2:
            e_copy(m, -1, 2, xp).wait_send()
        else:
            e_copy(m, 1, 2, xm).wait_send()
        for k in range(NX):
            to_core(m, k).wait_send()
    for j in range(CHUNKS):
        for way in range(2):
            w_copy(j, way).wait_send()
            w_forward(j, way).wait_send()


def shards(grams, weights):
    sub = grams.reshape(M, R, 4, R).transpose(2, 0, 1, 3)
    sub = jnp.pad(sub, ((0, 0), (0, 0), (0, 0), (0, LANES - R)))
    block = jax.ShapeDtypeStruct((R, CHUNKS * LANES), F32)
    vmem = pl.BlockSpec(memory_space=pltpu.VMEM)
    dma = pltpu.SemaphoreType.DMA
    return pl.pallas_call(
        kernel,
        out_shape=(block, block),
        in_specs=[vmem, vmem],
        out_specs=(vmem, vmem),
        scratch_shapes=[
            pltpu.VMEM((2, NX, M, HALF, LANES), BF16),
            pltpu.VMEM((HALF, 2 * HALF), BF16),
            pltpu.VMEM((HALF, 2 * HALF), BF16),
            pltpu.VMEM((M + 1, R, LANES), F32),
            pltpu.VMEM((CHUNKS, NY, M, LANES, LANES), BF16),
            pltpu.VMEM((CHUNKS, NZ, R, LANES), F32),
            pltpu.VMEM((2, CHUNKS, 4, R, LANES), F32),
            pltpu.VMEM((CHUNKS, 2 * HALF, LANES), BF16),
            pltpu.VMEM((CHUNKS, 2 * HALF, LANES), BF16),
            pltpu.VMEM((2, CHUNKS, NY, R, LANES), F32),
            pltpu.VMEM((2, 2, CHUNKS, 2, R, LANES), F32),
            pltpu.VMEM((CHUNKS, R, LANES), F32),
            pltpu.VMEM((CHUNKS, R, LANES), F32),
            pltpu.VMEM((CHUNKS, R, LANES), F32),
            pltpu.VMEM((CHUNKS, R, LANES), F32),
            pltpu.VMEM((2, CHUNKS, NY, 4, LANES), F32),
            pltpu.VMEM((2, CHUNKS, NZ, 4, LANES), F32),
            dma((M, 4)),
            dma((M, 4)),
            dma((7, M)),
            dma((7, M)),
            dma((4, CHUNKS)),
            dma((4, CHUNKS)),
            dma((KINDS,)),
            dma((KINDS, CHUNKS)),
        ],
        compiler_params=pltpu.CompilerParams(
            collective_id=0, has_side_effects=True, vmem_limit_bytes=56 * 1024 * 1024
        ),
    )(sub, weights)


def solution(mesh):
    torus = Mesh(mesh.devices.reshape(NY, NZ, NX, 2), ("y", "z", "x", "c"))
    spec = P(None, ("y", "z"), ("x", "c"))
    out = P(("y", "z"), ("x", "c"))
    return jax.shard_map(shards, mesh=torus, in_specs=(spec, spec), out_specs=(out, out), check_vma=False)
```

```python
import functools

import jax
import jax.numpy as jnp
from jax import lax
from jax.experimental import pallas as pl
from jax.experimental.pallas import tpu as pltpu
from jax.sharding import Mesh
from jax.sharding import PartitionSpec as P

MESH = pl.DeviceIdType.MESH
F32 = jnp.float32
BF16 = jnp.bfloat16

NX, NY, NZ = 4, 4, 8
M = 4
R = 112
LANES = 128
HALF = 4 * R
CHUNKS = 7
F_LO, F_HI = pl.ds(0, 56), pl.ds(56, 56)

GATHER = ("ring", "hybrid")
RSY_DIRECT = True
DELAY_RIGHT = (0, 0, 0, 0, 0)
DELAY = ((0, 0, 0, 0, 0, 0, 0), (0, 0, 0, 0, 0))
STAGES = 20


def kernel(
    g_ref,
    w_ref,
    merged_ref,
    resid_ref,
    gt,
    t_hi,
    t_lo,
    diag,
    wb,
    cb,
    rz,
    d1,
    d2,
    pb,
    ry,
    res,
    dirn,
    mapped,
    merged,
    sty,
    stz,
    q_send,
    q_recv,
    e_send,
    e_recv,
    core_recv,
    w_send,
    w_recv,
    s_send,
    s_recv,
):
    x, y, z, c = (lax.axis_index(a) for a in ("x", "y", "z", "c"))
    other = 1 - c
    z_half, z_quarter = lax.div(z, 4), lax.rem(z, 4)
    home = z_half == c

    def at(axis, index, step, size):
        return {axis: lax.rem(index + (step + size), size)}

    xp, xm = at("x", x, 1, NX), at("x", x, -1, NX)
    yp, ym = at("y", y, 1, NY), at("y", y, -1, NY)
    zp, zm = at("z", z, 1, NZ), at("z", z, -1, NZ)

    def zi(step):
        return lax.rem(z + (step + NZ), NZ)

    def yi(step):
        return lax.rem(y + (step + NY), NY)

    def xi(step):
        return lax.rem(x + (step + NX), NX)

    def copy(src, dst, send, recv, device):
        return pltpu.make_async_remote_copy(
            src_ref=src, dst_ref=dst, send_sem=send, recv_sem=recv, device_id=device, device_id_type=MESH
        )

    barrier = pltpu.get_barrier_semaphore()
    for dz in range(NZ):
        for dc in range(2):
            if dz or dc:
                pl.semaphore_signal(
                    barrier, inc=1, device_id={"z": zi(dz), "c": lax.rem(c + dc, 2)}, device_id_type=MESH
                )
    for d in (1, 2, 3):
        pl.semaphore_signal(barrier, inc=1, device_id=at("y", y, d, NY), device_id_type=MESH)
    for device in (xp, xm):
        pl.semaphore_signal(barrier, inc=1, device_id=device, device_id_type=MESH)
    pl.semaphore_wait(barrier, 2 * NZ - 1 + 3 + 2)

    def w_copy(j, way):
        lanes = pl.ds(j * LANES, LANES)
        return copy(
            w_ref.at[:, :, lanes], wb.at[j, y, :, pl.ds(0, R), :], w_send.at[way], w_recv.at[way, j], (yp, ym)[way]
        )

    def w_arrival(j, way):
        dst = wb.at[j, yi(-1 if way == 0 else 1), :, pl.ds(0, R), :]
        return copy(dst, dst, w_send.at[way], w_recv.at[way, j], (yp, ym)[way])

    def w_forward(j, way):
        models = pl.ds(0, 2) if way == 0 else pl.ds(2, 2)
        dst = wb.at[j, yi(-1 if way == 0 else 1), models, pl.ds(0, R), :]
        return copy(dst, dst, w_send.at[2 + way], w_recv.at[2 + way, j], (yp, ym)[way])

    def w_far(j, way):
        models = pl.ds(0, 2) if way == 0 else pl.ds(2, 2)
        dst = wb.at[j, yi(2), models, pl.ds(0, R), :]
        return copy(dst, dst, w_send.at[2 + way], w_recv.at[2 + way, j], (yp, ym)[way])

    def q_copy(m, quarter):
        return copy(
            g_ref.at[quarter, m],
            gt.at[z_half, x, m, pl.ds(pl.multiple_of(z_quarter * R, 16), R), :],
            q_send.at[0],
            q_recv.at[m],
            {"z": 4 * c + quarter, "c": z_half},
        )

    def q_take(m):
        for blocks, there in ((3, home), (4, jnp.logical_not(home))):

            @pl.when(there)
            def _():
                dst = gt.at[c, x, m, pl.ds(0, blocks * R), :]
                copy(dst, dst, q_send.at[0], q_recv.at[m], zp).wait_recv()

    def away(quarter):
        return jnp.logical_not(jnp.logical_and(home, z_quarter == quarter))

    for m in range(M):
        for quarter in range(4):

            @pl.when(away(quarter))
            def _():
                q_copy(m, quarter).start()

    for j in range(CHUNKS):
        for way in range(2):
            w_copy(j, way).start()

    @pl.when(home)
    def _():
        rows = pl.ds(pl.multiple_of(z_quarter * R, 16), R)
        for m in range(M):
            gt[z_half, x, m, rows, :] = g_ref[z_quarter, m]

    for j in range(CHUNKS):
        for m in range(M):
            wb[j, y, m, pl.ds(0, R), :] = w_ref[m, :, j * LANES : (j + 1) * LANES]
            for k in range(NY):
                wb[j, k, m, pl.ds(R, LANES - R), :] = jnp.zeros((LANES - R, LANES), BF16)

    def e_copy(m, offset, kind, device):
        ref = gt.at[c, xi(offset), m]
        return copy(ref, ref, e_send.at[0], e_recv.at[kind, m], device)

    def to_core(m, k):
        ref = gt.at[c, xi(k), m]
        return copy(ref, ref, e_send.at[1], core_recv.at[0], {"c": other})

    for m in range(M):
        q_take(m)
        e_copy(m, 0, 0, xp).start()
        e_copy(m, 0, 1, xm).start()
        to_core(m, 0).start()
    for j in range(2):
        for way in range(2):
            w_arrival(j, way).wait_recv()
            w_forward(j, way).start()
    for m in (0, 2, 1, 3):
        e_copy(m, -1, 0, xp).wait_recv()
        if m < 2:
            e_copy(m, -1, 2, xp).start()
        to_core(m, 3).start()
        e_copy(m, 1, 1, xm).wait_recv()
        if m >= 2:
            e_copy(m, 1, 2, xm).start()
        to_core(m, 1).start()
    for j in range(2, CHUNKS):
        for way in range(2):
            w_arrival(j, way).wait_recv()
            w_forward(j, way).start()
    for m in (0, 2, 1, 3):
        e_copy(m, 2, 2, xp).wait_recv()
        to_core(m, 2).start()
    from_core = gt.at[other]
    copy(from_core, from_core, e_send.at[1], core_recv.at[0], {"c": other}).wait_recv()

    for k in range(NX):
        total = jnp.concatenate(
            [
                gt[h, k, 0].astype(F32) + gt[h, k, 1].astype(F32) + gt[h, k, 2].astype(F32) + gt[h, k, 3].astype(F32)
                for h in range(2)
            ],
            axis=0,
        )
        total = jnp.transpose(total)[:R]
        high = total.astype(BF16)
        t_hi[k * R : (k + 1) * R, :] = high
        t_lo[k * R : (k + 1) * R, :] = (total - high.astype(F32)).astype(BF16)
    on_diag = lax.broadcasted_iota(jnp.int32, (R, LANES), 0) == lax.broadcasted_iota(jnp.int32, (R, LANES), 1)
    diag_total = jnp.zeros((R, LANES), F32)
    for m in range(M):
        block = gt[z_half, y, m, pl.ds(pl.multiple_of(z_quarter * R, 16), R), :].astype(F32)
        values = jnp.sum(jnp.where(on_diag, block, 0.0), axis=1, keepdims=True)
        values = jnp.broadcast_to(values, (R, LANES))
        diag[m] = values
        diag_total = diag_total + values
    diag[M] = diag_total

    def slot(stage, j):
        return 4 * stage + lax.rem(j, 4)

    def send(stage, j, messages):
        for ref, dst, device in messages:
            copy(ref, dst, s_send.at[slot(stage, j)], s_recv.at[slot(stage, j)], device).start()

    def take(stage, j, whole):
        both = copy(whole, whole, s_send.at[slot(stage, j)], s_recv.at[slot(stage, j)], zp)
        both.wait_recv()
        both.wait_send()

    def own_rows(index):
        return pl.multiple_of(index * R, 16)

    def rsz_send(stage, step, j):
        messages = []
        for way in range(2):
            t = zi((5 - step) if way == 0 else (step - 5))
            rows = pl.ds(0, R) if step > 1 else (F_LO, F_HI)[way]
            messages.append((cb.at[j, t, rows, :], rz.at[way, j, step - 1, rows, :], (zp, zm)[way]))
        send(stage, j, messages)

    def right_partial(stage, j):
        for way in range(2):
            w_far(j, way).wait_recv()
        for h in range(2):
            acc = jnp.zeros((HALF, LANES), F32)
            for k in range(NY):
                for m in (0, 2):
                    lhs = jnp.concatenate([gt[h, k, m], gt[h, k, m + 1]], axis=1)
                    rhs = jnp.concatenate([wb[j, k, m], wb[j, k, m + 1]], axis=0)
                    acc = acc + jnp.dot(lhs, rhs, preferred_element_type=F32)
            for q in range(4):
                cb[j, 4 * h + q] = acc[q * R : (q + 1) * R]
        rsz_send(stage, 1, j)

    def right_step(step, stage, j):
        take(stage - 1, j, cb.at[j, 0] if step == 2 else cb.at[j, pl.ds(0, 2)])
        plus, minus = zi(5 - step), zi(step - 5)
        if step == 2:
            cb[j, plus, F_LO, :] += rz[0, j, 0, F_LO, :]
            cb[j, minus, F_HI, :] += rz[1, j, 0, F_HI, :]
        else:
            cb[j, plus] += rz[0, j, step - 2]
            cb[j, minus] += rz[1, j, step - 2]
        rsz_send(stage, step, j)

    def d_rows(it, j, step, first=0, count=R):
        return (d1, d2)[it].at[j, pl.ds(pl.multiple_of(zi(step) * R + first, 16), count), :]

    def same(ref, device):
        return ref, ref, device

    LO, HI = (0, 64), (64, 48)
    zpp, zmm = at("z", z, 2, NZ), at("z", z, -2, NZ)

    def gather_start(it, stage, j):
        own = d_rows(it, j, 0)
        devices = [zp, zm]
        if GATHER[it] == "hybrid":
            devices += [zpp, zmm]
        elif GATHER[it] == "direct":
            devices = [at("z", z, d, NZ) for d in (4, 3, -3, 2, -2, 1, -1)]
        send(stage, j, [same(own, device) for device in devices])

    def gather_steps(it):
        ref = (d1, d2)[it]

        def ring(step, stage, j):
            take(stage - 1, j, ref.at[j, pl.ds(0, 2 * R), :])
            near, far = (1 - step, step - 1)
            parts = (LO, HI) if step == 4 else ((0, R), (0, R))
            send(stage, j, [same(d_rows(it, j, near, *parts[0]), zp), same(d_rows(it, j, far, *parts[1]), zm)])

        def hybrid(stage, j):
            take(stage - 1, j, ref.at[j, pl.ds(0, 4 * R), :])
            send(
                stage,
                j,
                [
                    same(d_rows(it, j, -2), zp),
                    same(d_rows(it, j, 2), zm),
                    same(d_rows(it, j, -2, *LO), zpp),
                    same(d_rows(it, j, 2, *HI), zmm),
                ],
            )

        if GATHER[it] == "ring":
            return [functools.partial(ring, step) for step in (2, 3, 4)], R
        if GATHER[it] == "hybrid":
            return [hybrid], 3 * R
        return [], 7 * R

    def right_end(stage, j):
        take(stage - 1, j, cb.at[j, pl.ds(0, 2)])
        product = cb[j, z] + rz[0, j, 3] + rz[1, j, 3]
        on_diag_sum = jnp.zeros((R, LANES), F32)
        for m in range(M):
            on_diag_sum = on_diag_sum + diag[m] * wb[j, y, m, pl.ds(0, R), :].astype(F32)
        right = 0.9 * product + 0.1 * on_diag_sum
        res[j] = right
        dirn[j] = right
        d1[j, pl.ds(own_rows(z), R), :] = right.astype(BF16)
        gather_start(0, stage, j)

    def map_partial(it, last_rows, stage, j):
        ref = (d1, d2)[it]
        take(stage - 1, j, ref.at[j, pl.ds(0, last_rows), :])
        d = ref[j]
        out = jnp.dot(t_hi[...], d, preferred_element_type=F32) + jnp.dot(t_lo[...], d, preferred_element_type=F32)
        for q in range(NY):
            pb[it, j, q] = out[q * R : (q + 1) * R]
        if RSY_DIRECT:
            send(
                stage,
                j,
                [(pb.at[it, j, yi(d)], ry.at[it, j, d - 1], at("y", y, d, NY)) for d in (2, 1, 3)],
            )
        else:
            t = yi(2)
            send(
                stage,
                j,
                [
                    (pb.at[it, j, t, F_LO, :], ry.at[it, j, 1, F_LO, :], yp),
                    (pb.at[it, j, t, F_HI, :], ry.at[it, j, 1, F_HI, :], ym),
                ],
            )

    def map_step(it, stage, j):
        take(stage - 1, j, pb.at[it, j, 0])
        pb[it, j, yi(1), F_LO, :] += ry[it, j, 1, F_LO, :]
        pb[it, j, yi(-1), F_HI, :] += ry[it, j, 1, F_HI, :]
        send(
            stage,
            j,
            [(pb.at[it, j, yi(1)], ry.at[it, j, 0], yp), (pb.at[it, j, yi(-1)], ry.at[it, j, 2], ym)],
        )

    def map_end(it, stage, j):
        take(stage - 1, j, pb.at[it, j, pl.ds(0, 3 if RSY_DIRECT else 2)])
        product = pb[it, j, y] + ry[it, j, 0] + ry[it, j, 2]
        if RSY_DIRECT:
            product = product + ry[it, j, 1]
        rounded = (d1, d2)[it][j, pl.ds(own_rows(z), R), :].astype(F32)
        value = 0.9 * product + 0.1 * diag[M] * rounded
        mapped[j] = value
        r = res[j]
        norm = jnp.sum(r * r, axis=0, keepdims=True)
        curvature = jnp.sum(dirn[j] * value, axis=0, keepdims=True)
        square = jnp.sum(value * value, axis=0, keepdims=True)
        cross = jnp.sum(r * value, axis=0, keepdims=True)
        sty[it, j, y] = jnp.concatenate([norm, curvature, square, cross], axis=0)
        send(stage, j, [same(sty.at[it, j, y], at("y", y, d, NY)) for d in (2, 1, 3)])

    def sum_z(it, stage, j):
        take(stage - 1, j, sty.at[it, j, pl.ds(0, NY - 1)])
        stz[it, j, z] = (sty[it, j, 0] + sty[it, j, 1]) + (sty[it, j, 2] + sty[it, j, 3])
        send(stage, j, [same(stz.at[it, j, z], at("z", z, d, NZ)) for d in (4, 3, 5, 2, 6, 1, 7)])

    def update(it, stage, j):
        take(stage - 1, j, stz.at[it, j, pl.ds(0, NZ - 1)])
        sums = stz[it, j, 0]
        for k in range(1, NZ):
            sums = sums + stz[it, j, k]
        norm, curvature, square, cross = (sums[k : k + 1] for k in range(4))
        step = norm / curvature
        direction = dirn[j]
        residual = res[j] - step * mapped[j]
        if it == 0:
            norm_next = norm - 2.0 * step * cross + step * step * square
            merged[j] = step * direction
            direction = residual + norm_next / norm * direction
            res[j] = residual
            dirn[j] = direction
            d2[j, pl.ds(own_rows(z), R), :] = direction.astype(BF16)
            gather_start(1, stage, j)
        else:
            lanes = pl.ds(pl.multiple_of(j * LANES, LANES), LANES)
            merged_ref[:, lanes] = merged[j] + step * direction
            resid_ref[:, lanes] = residual

    stages = [right_partial]
    stages += [functools.partial(right_step, step) for step in (2, 3, 4)]
    stages += [right_end]
    delays = list(DELAY_RIGHT)
    for it in range(2):
        steps, last_rows = gather_steps(it)
        stages += steps
        stages += [functools.partial(map_partial, it, last_rows)]
        if not RSY_DIRECT:
            stages += [functools.partial(map_step, it)]
        stages += [functools.partial(f, it) for f in (map_end, sum_z, update)]
        delays += list(DELAY[it])
    assert len(stages) == len(delays) + 0
    ticks = [s + sum(delays[:s]) for s in range(len(stages))]

    def tick(t, carry):
        for s in range(len(stages)):
            j = t - ticks[s]

            @pl.when(jnp.logical_and(j >= 0, j < CHUNKS))
            def _():
                stages[s](s, j)

        return carry

    lax.fori_loop(0, CHUNKS + ticks[-1], tick, 0)

    for blocks, there in ((3, home), (4, jnp.logical_not(home))):

        @pl.when(there)
        def _():
            ref = g_ref.at[pl.ds(0, blocks)]
            copy(ref, ref, q_send.at[0], q_recv.at[0], zp).wait_send()

    along_x = gt.at[0, pl.ds(0, 3)]
    copy(along_x, along_x, e_send.at[0], e_recv.at[0, 0], xp).wait_send()
    copy(from_core, from_core, e_send.at[1], core_recv.at[0], {"c": other}).wait_send()
    for way in range(2):
        copy(w_ref, w_ref, w_send.at[way], w_recv.at[way, 0], yp).wait_send()
        ref = w_ref.at[pl.ds(0, 2)]
        copy(ref, ref, w_send.at[2 + way], w_recv.at[2 + way, 0], yp).wait_send()


def shards(grams, weights):
    sub = grams.reshape(M, R, 4, R).transpose(2, 0, 1, 3)
    sub = jnp.pad(sub, ((0, 0), (0, 0), (0, 0), (0, LANES - R)))
    block = jax.ShapeDtypeStruct((R, CHUNKS * LANES), F32)
    vmem = pl.BlockSpec(memory_space=pltpu.VMEM)
    dma = pltpu.SemaphoreType.DMA
    return pl.pallas_call(
        kernel,
        out_shape=(block, block),
        in_specs=[vmem, vmem],
        out_specs=(vmem, vmem),
        scratch_shapes=[
            pltpu.VMEM((2, NX, M, HALF, LANES), BF16),
            pltpu.VMEM((HALF, 2 * HALF), BF16),
            pltpu.VMEM((HALF, 2 * HALF), BF16),
            pltpu.VMEM((M + 1, R, LANES), F32),
            pltpu.VMEM((CHUNKS, NY, M, LANES, LANES), BF16),
            pltpu.VMEM((CHUNKS, NZ, R, LANES), F32),
            pltpu.VMEM((2, CHUNKS, 4, R, LANES), F32),
            pltpu.VMEM((CHUNKS, 2 * HALF, LANES), BF16),
            pltpu.VMEM((CHUNKS, 2 * HALF, LANES), BF16),
            pltpu.VMEM((2, CHUNKS, NY, R, LANES), F32),
            pltpu.VMEM((2, CHUNKS, 3, R, LANES), F32),
            pltpu.VMEM((CHUNKS, R, LANES), F32),
            pltpu.VMEM((CHUNKS, R, LANES), F32),
            pltpu.VMEM((CHUNKS, R, LANES), F32),
            pltpu.VMEM((CHUNKS, R, LANES), F32),
            pltpu.VMEM((2, CHUNKS, NY, 4, LANES), F32),
            pltpu.VMEM((2, CHUNKS, NZ, 4, LANES), F32),
            dma((1,)),
            dma((M,)),
            dma((2,)),
            dma((3, M)),
            dma((1,)),
            dma((4,)),
            dma((4, CHUNKS)),
            dma((4 * STAGES,)),
            dma((4 * STAGES,)),
        ],
        compiler_params=pltpu.CompilerParams(
            collective_id=0, has_side_effects=True, vmem_limit_bytes=56 * 1024 * 1024
        ),
    )(sub, weights)


def solution(mesh):
    torus = Mesh(mesh.devices.reshape(NY, NZ, NX, 2), ("y", "z", "x", "c"))
    spec = P(None, ("y", "z"), ("x", "c"))
    out = P(("y", "z"), ("x", "c"))
    return jax.shard_map(shards, mesh=torus, in_specs=(spec, spec), out_specs=(out, out), check_vma=False)
```
